32 devices in a mesh: ma: 16 (over z, x, core), af: 2 (over y).
Axes of the slice: x: 2, y: 2, z: 4, core: 2. Of those that a mesh axis runs over, the one named last changes fastest.
Arguments:
- coeffs: bfloat16 [512, 128, 2049], P('ma', 'af'), parts along dimension 1, may hold values from -6 to 6
- legendre: bfloat16 [512, 256, 2049], P('ma'), may hold values from -0.1875 to 0.1875
- assign: int32 [512], P('ma'), may hold values from 0 to 511, each once
Outputs:
- fourier: float32 [512, 128, 1024], P('ma', 'af'), parts along dimension 1
The draws below stay inside these ranges and needn't reach their ends.
There are 2 independent parts, one for each index of `af`. The reference program is written for one: setup_inputs(seed, part) draws one part's arguments, and reference() takes and returns one part's arrays. A program takes and returns all parts, laid end to end along the dimension named above; an argument that names none is the same for every part. Nothing has to cross between parts.
Inputs may be any that keep to these rules, and one draw needn't show every extreme that they name: Slot s carries the wavenumbers assign[s] and 2047 - assign[s]; every pair appears once.
All inputs are finite; a program needn't handle non-finite values.
Results may differ from the reference program's by a relative error of at most 0.0003.
Values sent between devices are 32-bit elements; how exact they have to be, the bound alone decides.
No kernel may reach another device: no remote copies, remote signals or barrier semaphores. Data moves between devices by JAX's collectives and lax.ppermute only.
A program may use at most 128 MiB of HBM per device.

```python
import jax
import jax.numpy as jnp
from jax import lax

TRUNC = 2047
PAIRS = 512
HLAT = 256
FIELDS = 32
KP = 2049
COLS = 64


def block_scale(key, extent, pieces, low, high):
    level, own = 1.0, jax.random.fold_in(key, 6)
    for dim, blocks in pieces:
        heights = jnp.exp(jax.random.uniform(jax.random.fold_in(own, dim), (blocks,), jnp.float32, low / len(pieces), high / len(pieces)))
        level = level * jnp.repeat(heights, extent[dim] // blocks).reshape([-1 if axis == dim else 1 for axis in range(len(extent))])
    return level


def centred(rng, shape, scale, most, shards=(), held_as=jnp.bfloat16):
    gain = block_scale(rng, shape, shards, -0.22, 0.18) if shards else 1.0
    entries = jax.random.normal(rng, shape, jnp.float32) * scale * gain
    return jnp.minimum(jnp.maximum(entries, -most), most).astype(held_as)


def setup_inputs(seed: int = 0, part: int = 0) -> dict:
    seeds = jax.random.split(jax.random.key(seed), 4)
    part_keys = jax.random.split(jax.random.fold_in(seeds[3], part), 4)
    coeffs = centred(part_keys[0], (PAIRS, COLS, KP), 1.0, 6.0, ((0, 16),))
    legendre = centred(seeds[1], (PAIRS, HLAT, KP), (KP // 2) ** -0.5, 0.1875, ((0, 16),))
    assign = jax.random.permutation(seeds[2], PAIRS).astype(jnp.int32)
    return {"coeffs": coeffs, "legendre": legendre, "assign": assign}


def slot_values(legendre_rows, coeff_rows, pair):
    entry = jnp.arange(KP, dtype=jnp.int32)
    first_len = (TRUNC + 1 - pair).astype(jnp.int32)
    second = entry >= first_len
    degree_gap = jnp.where(second, entry - first_len, entry)
    odd_gap = (degree_gap % 2) == 1
    group_masks = jnp.stack([
        jnp.logical_and(jnp.logical_not(second), jnp.logical_not(odd_gap)),
        jnp.logical_and(jnp.logical_not(second), odd_gap),
        jnp.logical_and(second, jnp.logical_not(odd_gap)),
        jnp.logical_and(second, odd_gap)], axis=0).astype(jnp.float32)
    masked = coeff_rows.astype(jnp.float32)[None, :, :] * group_masks[:, None, :]
    partial_value = jnp.einsum('hk,gck->hcg', legendre_rows.astype(jnp.float32), masked)
    north_rows = partial_value[:, :, 0::2] + partial_value[:, :, 1::2]
    south_rows = partial_value[:, :, 0::2] - partial_value[:, :, 1::2]
    return jnp.concatenate([north_rows, south_rows[::-1]], axis=0)


def reference(coeffs, legendre, assign):
    def one_slot(items):
        return slot_values(items[0], items[1], items[2])

    values = lax.map(one_slot, (legendre, coeffs, assign))
    values = jnp.transpose(values, (1, 2, 0, 3)).reshape(2 * HLAT, 2 * FIELDS, 2 * PAIRS)
    column = jnp.arange(2 * PAIRS, dtype=jnp.int32)
    owner_pair = assign[column // 2]
    column_place = jnp.where(column % 2 == 0, owner_pair, 2 * PAIRS - 1 - owner_pair).astype(jnp.int32)
    fourier = jnp.zeros((2 * HLAT, 2 * FIELDS, 2 * PAIRS), jnp.float32)
    return fourier.at[:, :, column_place].set(values)
```

```python
import jax
import jax.numpy as jnp
from jax import lax
from jax.experimental import pallas as pl
from jax.experimental.pallas import tpu as pltpu
from jax.sharding import PartitionSpec as P

TRUNC = 2047
CHUNK = 8
ROWS = 8


def bands_kernel(pair_ref, coeffs_ref, legendre_ref, out_ref, wide_ref, turned_ref, last_ref):
    width, slots, lats = legendre_ref.shape
    main = width - 1
    columns = coeffs_ref.shape[1]
    devices, _, band, _ = out_ref.shape
    half = devices // 2
    block = wide_ref.shape[0]

    def turn(step, carry):
        rows = pl.ds(pl.multiple_of(step * block, block), block)
        wide_ref[...] = legendre_ref[rows].astype(jnp.float32)
        for slot in range(slots):
            turned_ref[slot, rows, :] = wide_ref[:, slot, :].astype(jnp.bfloat16)
        return carry

    lax.fori_loop(0, main // block, turn, 0)
    last_ref[...] = legendre_ref[main].astype(jnp.float32)

    def one_slot(slot, carry):
        pair = pair_ref[slot]
        first_len = TRUNC + 1 - pair
        value = coeffs_ref[slot].astype(jnp.float32)
        entry = lax.broadcasted_iota(jnp.int32, value.shape, 1)
        second = entry >= first_len
        gap = jnp.where(second, entry - first_len, entry)
        signed = jnp.where((gap & 1) == 1, -value, value)
        groups = [
            jnp.where(second, 0.0, value),
            jnp.where(second, value, 0.0),
            jnp.where(second, 0.0, signed),
            jnp.where(second, signed, 0.0),
        ]
        weights = jnp.concatenate(groups, axis=0)
        total = jnp.dot(
            weights[:, :main].astype(jnp.bfloat16), turned_ref[slot], preferred_element_type=jnp.float32
        )
        total = total + weights[:, main:] * last_ref[pl.ds(slot, 1), :]
        total = total.T
        for place in range(half):
            rows = total[place * band : (place + 1) * band]
            out_ref[place, slot] = rows[:, : 2 * columns]
            out_ref[devices - 1 - place, slot] = rows[:, 2 * columns :]
        return carry

    lax.fori_loop(0, slots, one_slot, 0)


def bands(coeffs, turned, pair_ids, chunk, devices):
    columns, width = coeffs.shape[1:]
    lats = turned.shape[2]
    band = 2 * lats // devices
    shape = (devices, CHUNK, band, 2 * columns)
    return pl.pallas_call(
        bands_kernel,
        grid_spec=pltpu.PrefetchScalarGridSpec(
            num_scalar_prefetch=1,
            grid=(1,),
            in_specs=[
                pl.BlockSpec((CHUNK, columns, width), lambda i, s: (chunk, 0, 0)),
                pl.BlockSpec((width, CHUNK, lats), lambda i, s: (0, chunk, 0)),
            ],
            out_specs=pl.BlockSpec(shape, lambda i, s: (0, 0, 0, 0)),
            scratch_shapes=[
                pltpu.VMEM((128, CHUNK, lats), jnp.float32),
                pltpu.VMEM((CHUNK, width - 1, lats), jnp.bfloat16),
                pltpu.VMEM((CHUNK, lats), jnp.float32),
            ],
        ),
        out_shape=jax.ShapeDtypeStruct(shape, jnp.float32),
        compiler_params=pltpu.CompilerParams(vmem_limit_bytes=56 * 1024 * 1024),
        cost_estimate=pl.CostEstimate(
            flops=2 * CHUNK * lats * width * 4 * columns,
            bytes_accessed=2 * CHUNK * width * (lats + columns) + 4 * devices * CHUNK * band * 2 * columns,
            transcendentals=0,
        ),
        name="bands",
    )(pair_ids, coeffs, turned)


def place_kernel(south_ref, low_ref, high_ref, *refs):
    *received, out_ref = refs
    rows, columns, total = out_ref.shape
    half = total // 2
    south = south_ref[0]
    low, high = [], []
    for row in range(rows):
        pieces = [ref[:, :, row, :] for ref in received]
        pieces = [piece.reshape(-1, piece.shape[-1]).T for piece in pieces]
        value = jnp.concatenate(pieces, axis=1)
        low.append(value[:columns])
        high.append(value[columns:])
    for values, order_ref, start in ((low, low_ref, 0), (high, high_ref, half)):
        value = jnp.concatenate(values, axis=0)
        lead = value.astype(jnp.bfloat16)
        rest = (value - lead.astype(jnp.float32)).astype(jnp.bfloat16)
        order = order_ref[...]
        placed = jnp.dot(lead, order, preferred_element_type=jnp.float32)
        placed = placed + jnp.dot(rest, order, preferred_element_type=jnp.float32)
        for row in range(rows):
            target = jnp.where(south == 1, rows - 1 - row, row)
            out_ref[target, :, start : start + half] = placed[row * columns : (row + 1) * columns]


def place(received, pair_ids, south, lats, columns):
    pairs = pair_ids.shape[0]
    column = lax.broadcasted_iota(jnp.int32, (pairs, pairs), 1)
    low = (pair_ids[:, None] == column).astype(jnp.bfloat16)
    high = (pairs - 1 - pair_ids[:, None] == column).astype(jnp.bfloat16)
    steps = lats // ROWS

    def out_map(i, south_ref):
        return (jnp.where(south_ref[0] == 1, steps - 1 - i, i), 0, 0)

    whole = pl.BlockSpec((pairs, pairs), lambda i, s: (0, 0))
    pieces = [
        pl.BlockSpec((piece.shape[0], piece.shape[1], ROWS, piece.shape[3]), lambda i, s: (0, 0, i, 0))
        for piece in received
    ]
    return pl.pallas_call(
        place_kernel,
        grid_spec=pltpu.PrefetchScalarGridSpec(
            num_scalar_prefetch=1,
            grid=(steps,),
            in_specs=[whole, whole] + pieces,
            out_specs=pl.BlockSpec((ROWS, columns, 2 * pairs), out_map),
        ),
        out_shape=jax.ShapeDtypeStruct((lats, columns, 2 * pairs), jnp.float32),
        compiler_params=pltpu.CompilerParams(vmem_limit_bytes=48 * 1024 * 1024),
        name="place",
    )(south, low, high, *received)


def shards(coeffs, legendre, assign):
    devices = lax.axis_size("ma")
    me = lax.axis_index("ma")
    slots, columns, _ = coeffs.shape
    lats = 2 * legendre.shape[1] // devices
    all_pairs = lax.all_to_all(
        jnp.broadcast_to(assign[None, None, :], (devices, 1, slots)), "ma", 0, 0, tiled=True
    ).reshape(devices, slots)
    turned = jnp.transpose(legendre, (2, 0, 1))
    received, order = [], []
    for start in range(0, slots, CHUNK):
        stop = start + CHUNK
        sent = bands(coeffs, turned, assign[start:stop], start // CHUNK, devices)
        piece = lax.all_to_all(sent.reshape(devices, CHUNK * lats, 2 * columns), "ma", 0, 0, tiled=True)
        received.append(piece.reshape(devices, CHUNK, lats, 2 * columns))
        order.append(all_pairs[:, start:stop].reshape(-1))
    south = (me >= devices // 2).astype(jnp.int32).reshape(1)
    return place(received, jnp.concatenate(order), south, lats, columns)


def solution(mesh):
    return jax.shard_map(
        shards,
        mesh=mesh,
        in_specs=(P("ma", "af", None), P("ma", None, None), P("ma")),
        out_specs=P("ma", "af", None),
        check_vma=False,
    )
```

```python
import functools

import jax
import jax.numpy as jnp
from jax import lax
from jax.experimental import pallas as pl
from jax.experimental.pallas import tpu as pltpu
from jax.sharding import PartitionSpec as P

TRUNC = 2047
TILE = 8


def bands_kernel(chunk, extra, pair_ref, coeffs_ref, legendre_ref, *refs):
    if extra:
        pairs_ref, out_ref, wide_ref, turned_ref, last_ref = refs
    else:
        out_ref, wide_ref, turned_ref, last_ref = refs
    width, slots, lats = legendre_ref.shape
    main = width - 1
    columns = coeffs_ref.shape[1]
    devices = out_ref.shape[0]
    half = devices // 2
    band = lats // half
    parts = wide_ref.shape[0]
    block = wide_ref.shape[1] // slots
    first_slot = (chunk + pl.program_id(0)) * slots

    def turn(step, carry):
        rows = pl.ds(pl.multiple_of(step * block, block), block)
        wide = legendre_ref[rows].astype(jnp.float32).reshape(block * slots, lats)
        for part in range(parts):
            wide_ref[part] = wide[:, part * 128 : (part + 1) * 128]
        for slot in range(slots):
            value = jnp.concatenate(
                [
                    wide_ref[part, pl.ds(slot, block, stride=slots), :]
                    for part in range(parts)
                ],
                axis=1,
            )
            turned_ref[slot, rows, :] = value.astype(jnp.bfloat16)
        return carry

    lax.fori_loop(0, main // block, turn, 0)
    last_ref[...] = legendre_ref[main].astype(jnp.float32)

    def one_slot(slot, carry):
        first_len = TRUNC + 1 - pair_ref[first_slot + slot]
        value = coeffs_ref[slot].astype(jnp.float32)
        entry = lax.broadcasted_iota(jnp.int32, value.shape, 1)
        second = entry >= first_len
        gap = jnp.where(second, entry - first_len, entry)
        signed = jnp.where((gap & 1) == 1, -value, value)
        groups = [
            jnp.where(second, 0.0, value),
            jnp.where(second, value, 0.0),
            jnp.where(second, 0.0, signed),
            jnp.where(second, signed, 0.0),
        ]
        weights = jnp.concatenate(groups, axis=0)
        total = jnp.dot(
            weights[:, :main].astype(jnp.bfloat16), turned_ref[slot], preferred_element_type=jnp.float32
        )
        total = total + weights[:, main:] * last_ref[pl.ds(slot, 1), :]
        total = total.T
        for place in range(half):
            for group in range(band // TILE):
                start = place * band + group * TILE
                rows = total[start : start + TILE]
                for owner, part in (
                    (place, rows[:, : 2 * columns]),
                    (devices - 1 - place, rows[:, 2 * columns :]),
                ):
                    if extra:
                        at = pl.multiple_of((group * slots + slot) * TILE, TILE)
                        out_ref[owner, pl.ds(at, TILE), :] = part
                    else:
                        at = pl.multiple_of(slot * TILE, TILE)
                        out_ref[owner, group, pl.ds(at, TILE), :] = part
        return carry

    lax.fori_loop(0, slots, one_slot, 0)
    if extra:
        pairs = pairs_ref[...].astype(jnp.float32)
        row = out_ref.shape[1] - TILE
        for owner in range(devices):
            out_ref[owner, row : row + 1, : pairs.shape[1]] = pairs


def bands(coeffs, turned, assign, chunk, steps, devices):
    columns, width = coeffs.shape[1:]
    lats = turned.shape[2]
    groups = 2 * lats // devices // TILE
    extra = chunk == 0
    in_specs = [
        pl.BlockSpec((TILE, columns, width), lambda i, s: (chunk + i, 0, 0)),
        pl.BlockSpec((width, TILE, lats), lambda i, s: (0, chunk + i, 0)),
    ]
    operands = [assign, coeffs, turned]
    if extra:
        shape = (devices, (groups * TILE + 1) * TILE, 2 * columns)
        out_specs = pl.BlockSpec(shape, lambda i, s: (0, 0, 0))
        in_specs.append(pl.BlockSpec((1, assign.shape[0]), lambda i, s: (0, 0)))
        operands.append(assign.reshape(1, -1))
    else:
        shape = (devices, groups, steps * TILE * TILE, 2 * columns)
        out_specs = pl.BlockSpec((devices, groups, TILE * TILE, 2 * columns), lambda i, s: (0, 0, i, 0))
    return pl.pallas_call(
        functools.partial(bands_kernel, chunk, extra),
        grid_spec=pltpu.PrefetchScalarGridSpec(
            num_scalar_prefetch=1,
            grid=(steps,),
            in_specs=in_specs,
            out_specs=out_specs,
            scratch_shapes=[
                pltpu.VMEM((lats // 128, 128 * TILE, 128), jnp.float32),
                pltpu.VMEM((TILE, width - 1, lats), jnp.bfloat16),
                pltpu.VMEM((TILE, lats), jnp.float32),
            ],
        ),
        out_shape=jax.ShapeDtypeStruct(shape, jnp.float32),
        compiler_params=pltpu.CompilerParams(vmem_limit_bytes=56 * 1024 * 1024),
        cost_estimate=pl.CostEstimate(
            flops=2 * steps * TILE * lats * width * 4 * columns,
            bytes_accessed=2 * steps * TILE * width * (lats + columns),
            transcendentals=0,
        ),
        name="bands",
    )(*operands)


def place_kernel(south_ref, low_ref, high_ref, *refs):
    *received, out_ref = refs
    rows, columns, total = out_ref.shape
    half = total // 2
    south = south_ref[0]
    low, high = [], []
    for row in range(rows):
        pieces = []
        for ref in received:
            slots = ref.shape[-2] // rows
            for source in range(ref.shape[0]):
                picked = pl.ds(row, slots, stride=rows)
                pieces.append(ref[source, picked, :] if len(ref.shape) == 3 else ref[source, 0, picked, :])
        value = jnp.concatenate(pieces, axis=0).T
        low.append(value[:columns])
        high.append(value[columns:])
    for values, order_ref, start in ((low, low_ref, 0), (high, high_ref, half)):
        value = jnp.concatenate(values, axis=0)
        lead = value.astype(jnp.bfloat16)
        rest = (value - lead.astype(jnp.float32)).astype(jnp.bfloat16)
        order = order_ref[...]
        placed = jnp.dot(lead, order, preferred_element_type=jnp.float32)
        placed = placed + jnp.dot(rest, order, preferred_element_type=jnp.float32)
        for row in range(rows):
            target = jnp.where(south == 1, rows - 1 - row, row)
            out_ref[target, :, start : start + half] = placed[row * columns : (row + 1) * columns]


def place(received, pair_ids, south, lats, columns):
    pairs = pair_ids.shape[0]
    column = lax.broadcasted_iota(jnp.int32, (pairs, pairs), 1)
    low = (pair_ids[:, None] == column).astype(jnp.bfloat16)
    high = (pairs - 1 - pair_ids[:, None] == column).astype(jnp.bfloat16)
    steps = lats // TILE

    def out_map(i, south_ref):
        return (jnp.where(south_ref[0] == 1, steps - 1 - i, i), 0, 0)

    whole = pl.BlockSpec((pairs, pairs), lambda i, s: (0, 0))
    pieces = [
        pl.BlockSpec((piece.shape[0], TILE * TILE, piece.shape[2]), lambda i, s: (0, i, 0))
        if len(piece.shape) == 3
        else pl.BlockSpec((piece.shape[0], 1) + piece.shape[2:], lambda i, s: (0, i, 0, 0))
        for piece in received
    ]
    return pl.pallas_call(
        place_kernel,
        grid_spec=pltpu.PrefetchScalarGridSpec(
            num_scalar_prefetch=1,
            grid=(steps,),
            in_specs=[whole, whole] + pieces,
            out_specs=pl.BlockSpec((TILE, columns, 2 * pairs), out_map),
        ),
        out_shape=jax.ShapeDtypeStruct((lats, columns, 2 * pairs), jnp.float32),
        compiler_params=pltpu.CompilerParams(vmem_limit_bytes=48 * 1024 * 1024),
        name="place",
    )(south, low, high, *received)


def shards(coeffs, legendre, assign):
    devices = lax.axis_size("ma")
    me = lax.axis_index("ma")
    slots, columns, _ = coeffs.shape
    lats = 2 * legendre.shape[1] // devices
    turned = jnp.transpose(legendre, (2, 0, 1))
    tiles = slots // TILE
    received = []
    for chunk, steps in ((0, 1), (1, tiles - 1)):
        if steps:
            sent = bands(coeffs, turned, assign, chunk, steps, devices)
            flat = sent.reshape(devices, -1, 2 * columns)
            piece = lax.all_to_all(flat, "ma", 0, 0, tiled=True)
            received.append(piece.reshape(sent.shape))
    all_pairs = received[0][:, TILE * lats, :slots].astype(jnp.int32)
    order = [all_pairs[:, :TILE].reshape(-1), all_pairs[:, TILE:].reshape(-1)]
    south = (me >= devices // 2).astype(jnp.int32).reshape(1)
    return place(received, jnp.concatenate(order), south, lats, columns)


def solution(mesh):
    return jax.shard_map(
        shards,
        mesh=mesh,
        in_specs=(P("ma", "af", None), P("ma", None, None), P("ma")),
        out_specs=P("ma", "af", None),
        check_vma=False,
    )
```

```python
import functools

import jax
import jax.numpy as jnp
from jax import lax
from jax.experimental import pallas as pl
from jax.experimental.pallas import tpu as pltpu
from jax.sharding import PartitionSpec as P

TRUNC = 2047
TILE = 8


def bands_kernel(chunk, extra, pair_ref, coeffs_ref, legendre_ref, *refs):
    if extra:
        pairs_ref, out_ref, wide_ref, turned_ref, last_ref = refs
    else:
        out_ref, wide_ref, turned_ref, last_ref = refs
    width, slots, lats = legendre_ref.shape
    main = width - 1
    columns = coeffs_ref.shape[1]
    devices = out_ref.shape[0]
    half = devices // 2
    band = lats // half
    parts = wide_ref.shape[0]
    block = wide_ref.shape[1] // slots
    first_slot = (chunk + pl.program_id(0)) * slots

    def turn(step, carry):
        rows = pl.ds(pl.multiple_of(step * block, block), block)
        wide = legendre_ref[rows].astype(jnp.float32).reshape(block * slots, lats)
        for part in range(parts):
            wide_ref[part] = wide[:, part * 128 : (part + 1) * 128]
        for slot in range(slots):
            value = jnp.concatenate(
                [
                    wide_ref[part, pl.ds(slot, block, stride=slots), :]
                    for part in range(parts)
                ],
                axis=1,
            )
            turned_ref[slot, rows, :] = value.astype(jnp.bfloat16)
        return carry

    lax.fori_loop(0, main // block, turn, 0)
    last_ref[...] = legendre_ref[main].astype(jnp.float32)

    def one_slot(slot, carry):
        first_len = TRUNC + 1 - pair_ref[first_slot + slot]
        value = coeffs_ref[slot].astype(jnp.float32)
        entry = lax.broadcasted_iota(jnp.int32, value.shape, 1)
        second = entry >= first_len
        gap = jnp.where(second, entry - first_len, entry)
        signed = jnp.where((gap & 1) == 1, -value, value)
        groups = [
            jnp.where(second, 0.0, value),
            jnp.where(second, value, 0.0),
            jnp.where(second, 0.0, signed),
            jnp.where(second, signed, 0.0),
        ]
        weights = jnp.concatenate(groups, axis=0)
        total = jnp.dot(
            weights[:, :main].astype(jnp.bfloat16), turned_ref[slot], preferred_element_type=jnp.float32
        )
        total = total + weights[:, main:] * last_ref[pl.ds(slot, 1), :]
        total = total.T
        for place in range(half):
            for group in range(band // TILE):
                start = place * band + group * TILE
                rows = total[start : start + TILE]
                for owner, part in (
                    (place, rows[:, : 2 * columns]),
                    (devices - 1 - place, rows[:, 2 * columns :]),
                ):
                    if extra:
                        at = pl.multiple_of((group * slots + slot) * TILE, TILE)
                        out_ref[owner, pl.ds(at, TILE), :] = part
                    else:
                        at = pl.multiple_of(slot * TILE, TILE)
                        out_ref[owner, group, pl.ds(at, TILE), :] = part
        return carry

    lax.fori_loop(0, slots, one_slot, 0)
    if extra:
        pairs = pairs_ref[...].astype(jnp.float32)
        row = out_ref.shape[1] - TILE
        for owner in range(devices):
            out_ref[owner, row : row + 1, : pairs.shape[1]] = pairs


def bands(coeffs, turned, assign, chunk, steps, devices):
    columns, width = coeffs.shape[1:]
    lats = turned.shape[2]
    groups = 2 * lats // devices // TILE
    extra = chunk == 0
    in_specs = [
        pl.BlockSpec((TILE, columns, width), lambda i, s: (chunk + i, 0, 0)),
        pl.BlockSpec((width, TILE, lats), lambda i, s: (0, chunk + i, 0)),
    ]
    operands = [assign, coeffs, turned]
    if extra:
        shape = (devices, (groups * TILE + 1) * TILE, 2 * columns)
        out_specs = pl.BlockSpec(shape, lambda i, s: (0, 0, 0))
        in_specs.append(pl.BlockSpec((1, assign.shape[0]), lambda i, s: (0, 0)))
        operands.append(assign.reshape(1, -1))
    else:
        shape = (devices, groups, steps * TILE * TILE, 2 * columns)
        out_specs = pl.BlockSpec((devices, groups, TILE * TILE, 2 * columns), lambda i, s: (0, 0, i, 0))
    return pl.pallas_call(
        functools.partial(bands_kernel, chunk, extra),
        grid_spec=pltpu.PrefetchScalarGridSpec(
            num_scalar_prefetch=1,
            grid=(steps,),
            in_specs=in_specs,
            out_specs=out_specs,
            scratch_shapes=[
                pltpu.VMEM((lats // 128, 128 * TILE, 128), jnp.float32),
                pltpu.VMEM((TILE, width - 1, lats), jnp.bfloat16),
                pltpu.VMEM((TILE, lats), jnp.float32),
            ],
        ),
        out_shape=jax.ShapeDtypeStruct(shape, jnp.float32),
        compiler_params=pltpu.CompilerParams(vmem_limit_bytes=56 * 1024 * 1024),
        cost_estimate=pl.CostEstimate(
            flops=2 * steps * TILE * lats * width * 4 * columns,
            bytes_accessed=2 * steps * TILE * width * (lats + columns),
            transcendentals=0,
        ),
        name="bands",
    )(*operands)


def place_kernel(count, south_ref, low_ref, high_ref, *refs):
    received, out_ref = refs[:count], refs[-1]
    rows, columns, total = out_ref.shape
    half = total // 2
    south = south_ref[0]
    low, high = [], []
    for row in range(rows):
        pieces = []
        for ref in received:
            slots = ref.shape[-2] // rows
            for source in range(ref.shape[0]):
                picked = pl.ds(row, slots, stride=rows)
                pieces.append(ref[source, picked, :] if len(ref.shape) == 3 else ref[source, 0, picked, :])
        value = jnp.concatenate(pieces, axis=0).T
        low.append(value[:columns])
        high.append(value[columns:])
    for values, order_ref, start in ((low, low_ref, 0), (high, high_ref, half)):
        value = jnp.concatenate(values, axis=0)
        lead = value.astype(jnp.bfloat16)
        rest = (value - lead.astype(jnp.float32)).astype(jnp.bfloat16)
        order = order_ref[...]
        placed = jnp.dot(lead, order, preferred_element_type=jnp.float32)
        placed = placed + jnp.dot(rest, order, preferred_element_type=jnp.float32)
        for row in range(rows):
            target = jnp.where(south == 1, rows - 1 - row, row)
            out_ref[target, :, start : start + half] = placed[row * columns : (row + 1) * columns]


def orders(pair_ids):
    pairs = pair_ids.shape[0]
    column = lax.broadcasted_iota(jnp.int32, (pairs, pairs), 1)
    low = (pair_ids[:, None] == column).astype(jnp.bfloat16)
    high = (pairs - 1 - pair_ids[:, None] == column).astype(jnp.bfloat16)
    return low, high


def place(received, firsts, low, high, south, lats, columns, begin, end, out=None):
    pairs = low.shape[0]
    steps = lats // TILE

    def out_map(i, south_ref):
        return (jnp.where(south_ref[0] == 1, steps - 1 - begin - i, begin + i), 0, 0)

    whole = pl.BlockSpec((pairs, pairs), lambda i, s: (0, 0))
    pieces = [
        pl.BlockSpec((piece.shape[0], TILE * TILE, piece.shape[2]), lambda i, s, at=begin - first: (0, i + at, 0))
        if len(piece.shape) == 3
        else pl.BlockSpec(
            (piece.shape[0], 1) + piece.shape[2:], lambda i, s, at=begin - first: (0, i + at, 0, 0)
        )
        for piece, first in zip(received, firsts)
    ]
    before = [] if out is None else [out]
    return pl.pallas_call(
        functools.partial(place_kernel, len(received)),
        grid_spec=pltpu.PrefetchScalarGridSpec(
            num_scalar_prefetch=1,
            grid=(end - begin,),
            in_specs=[whole, whole] + pieces + [pl.BlockSpec(memory_space=pl.ANY) for _ in before],
            out_specs=pl.BlockSpec((TILE, columns, 2 * pairs), out_map),
        ),
        out_shape=jax.ShapeDtypeStruct((lats, columns, 2 * pairs), jnp.float32),
        compiler_params=pltpu.CompilerParams(vmem_limit_bytes=48 * 1024 * 1024),
        input_output_aliases={3 + len(received): 0} if before else {},
        name="place",
    )(south, low, high, *received, *before)


def shards(coeffs, legendre, assign):
    devices = lax.axis_size("ma")
    me = lax.axis_index("ma")
    slots, columns, _ = coeffs.shape
    lats = 2 * legendre.shape[1] // devices
    turned = jnp.transpose(legendre, (2, 0, 1))
    tiles = slots // TILE
    groups = lats // TILE

    def exchange(sent):
        flat = sent.reshape(devices, -1, 2 * columns)
        return lax.all_to_all(flat, "ma", 0, 0, tiled=True).reshape(sent.shape)

    lead = exchange(bands(coeffs, turned, assign, 0, 1, devices))
    all_pairs = lead[:, TILE * lats, :slots].astype(jnp.int32)
    low, high = orders(jnp.concatenate([all_pairs[:, :TILE].reshape(-1), all_pairs[:, TILE:].reshape(-1)]))
    south = (me >= devices // 2).astype(jnp.int32).reshape(1)
    if tiles == 1:
        return place([lead], [0], low, high, south, lats, columns, 0, groups)
    sent = bands(coeffs, turned, assign, 1, tiles - 1, devices)
    cut = max(groups - 1, 0)
    out, pieces = None, []
    for begin, end in ((0, cut), (cut, groups)):
        if end > begin:
            pieces.append((begin, end, exchange(sent[:, begin:end])))
    for begin, end, piece in pieces:
        out = place([lead, piece], [0, begin], low, high, south, lats, columns, begin, end, out)
    return out


def solution(mesh):
    return jax.shard_map(
        shards,
        mesh=mesh,
        in_specs=(P("ma", "af", None), P("ma", None, None), P("ma")),
        out_specs=P("ma", "af", None),
        check_vma=False,
    )
```
